128 devices in a mesh: seq: 64 (over y, z, x_lo, core), head: 2 (over x_hi).
Axes of the slice: x: 4 (x_hi: 2, x_lo: 2; x = x_hi * 2 + x_lo), y: 4, z: 4, core: 2. Of those that a mesh axis runs over, the one named last changes fastest.
Arguments:
- tokens: bfloat16 [32768, 2048], P('seq', 'head'), may hold values from -200 to 200
- norm_gain: float32 [2, 2048], replicated, may hold values from 0.25 to 1.75
- w_query: bfloat16 [2, 2048, 2048], P(None, None, 'head'), may hold values from -0.35 to 0.35
- key_projection_weight: bfloat16 [2, 2048, 512], P(None, None, 'head'), may hold values from -0.35 to 0.35
- value_projection_weight: bfloat16 [2, 2048, 512], P(None, None, 'head'), may hold values from -0.125 to 0.125
- w_out: bfloat16 [2, 2048, 2048], P(None, 'head'), may hold values from -0.125 to 0.125
- counts: int32 [64], replicated, may hold values from 128 to 512
Outputs:
- hidden_out: bfloat16 [32768, 2048], P('seq', 'head')
The draws below stay inside these ranges and needn't reach their ends.
Inputs may be any that keep to these rules, and one draw needn't show every extreme that they name: The first counts[b] tokens of block b of 512 positions are valid keys; the rest of the block is padding that no query uses as a key.
All inputs are finite; a program needn't handle non-finite values.
Results may differ from the reference program's by a relative error of at most 0.02.
The reference program's roundings to bfloat16 on the way count: a program that leaves them out, or rounds other values in their place, can miss the bound.
Values may be sent and summed in bfloat16 or wider, within the bound.
A program may use at most 128 MiB of HBM per device.

```python
import math
import jax
import jax.numpy as jnp
from jax import lax

MODEL_WIDTH = 2048
QUERY_HEAD_COUNT = 16
KEY_VALUE_HEADS = 4
HEAD_SIZE = 128
WINDOW = 4096
LAYER_COUNT = 2
BLOCK_TOKENS = 512
BLOCKS = 64
SEQUENCE_TOKENS = 32768
N_HEAD = 2


def sample_projection(key, salt, columns):
    scale_value = 1.6 / math.sqrt(MODEL_WIDTH)
    inner = jax.random.fold_in(key, salt)
    sampled_values = scale_value * jax.random.normal(inner, (LAYER_COUNT, MODEL_WIDTH, columns), jnp.float32)
    return jnp.clip(sampled_values, -0.35, 0.35)


def draw_w_query(key, part):
    sampled_values = sample_projection(key, 101, QUERY_HEAD_COUNT * HEAD_SIZE)
    return sampled_values.astype(jnp.bfloat16)


def draw_key_projection_weight(key, part):
    sampled_values = sample_projection(key, 102, KEY_VALUE_HEADS * HEAD_SIZE)
    return sampled_values.astype(jnp.bfloat16)


def draw_tokens(key, part):
    inner = jax.random.fold_in(key, 201)
    values = jnp.clip(jax.random.normal(inner, (SEQUENCE_TOKENS, MODEL_WIDTH), jnp.float32), -6.0, 6.0)
    return values.astype(jnp.bfloat16)


def set_ends(entries, rng, smallest, top_value):
    index_at = [jax.random.randint(jax.random.fold_in(rng, axis), (), 0, length) for axis, length in enumerate(entries.shape)]
    longest = entries.shape.index(max(entries.shape))
    next_to = index_at[:longest] + [(index_at[longest] + 1) % entries.shape[longest]] + index_at[longest + 1:]
    return entries.at[tuple(index_at)].set(smallest).at[tuple(next_to)].set(top_value)


def levels(key, dims, pieces, smallest, top_value):
    factor_of, own = 1.0, jax.random.fold_in(key, 6)
    for dim, shards_of in pieces:
        steps = jnp.exp(jax.random.uniform(jax.random.fold_in(own, dim), (shards_of,), jnp.float32, smallest / len(pieces), top_value / len(pieces)))
        factor_of = factor_of * jnp.repeat(steps, dims[dim] // shards_of).reshape([-1 if axis == dim else 1 for axis in range(len(dims))])
    return factor_of


def normal_values(stream_key, dims, width, most, pieces=(), kind=jnp.bfloat16):
    result = width * jax.random.normal(stream_key, dims, jnp.float32)
    if pieces:
        result = result * levels(stream_key, dims, pieces, -0.22, 0.18)
    return jnp.clip(result, -most, most).astype(kind)


def setup_inputs(seed: int = 0) -> dict:
    keys = jax.random.split(jax.random.key(seed), 8)
    return {
        "tokens": draw_tokens(jax.random.fold_in(keys[7], 71), 0),
        "norm_gain": jnp.clip(1.0 + 0.15 * jax.random.normal(keys[1], (LAYER_COUNT, MODEL_WIDTH), jnp.float32), 0.25, 1.75),
        "w_query": draw_w_query(jax.random.fold_in(keys[7], 71), 0),
        "key_projection_weight": draw_key_projection_weight(jax.random.fold_in(keys[7], 71), 0),
        "value_projection_weight": normal_values(keys[4], (LAYER_COUNT, MODEL_WIDTH, KEY_VALUE_HEADS * HEAD_SIZE), MODEL_WIDTH ** -0.5, 0.125, ((2, 2),)),
        "w_out": normal_values(keys[5], (LAYER_COUNT, QUERY_HEAD_COUNT * HEAD_SIZE, MODEL_WIDTH), (QUERY_HEAD_COUNT * HEAD_SIZE) ** -0.5, 0.125, ((1, 2),)),
        "counts": set_ends(jax.random.randint(keys[6], (BLOCKS,), BLOCK_TOKENS // 4, BLOCK_TOKENS + 1), jax.random.fold_in(keys[6], 1), BLOCK_TOKENS // 4, BLOCK_TOKENS).astype(jnp.int32),
    }


norm_epsilon = 1e-05
rope_base = 10000.0

def rms_norm(hidden, gain_row):
    widened = hidden.astype(jnp.float32)
    mean_square = lax.optimization_barrier(jnp.mean(widened * widened, axis=-1, keepdims=True))
    scaled = widened * lax.rsqrt(mean_square + norm_epsilon) * gain_row.astype(jnp.float32)
    return scaled.astype(jnp.bfloat16)

def apply_rotary_embedding(projected, token_positions, head_count):
    row_total = projected.shape[0]
    shaped = projected.reshape(row_total, head_count, HEAD_SIZE)
    half_dim = HEAD_SIZE // 2
    inverse = jnp.power(jnp.float32(rope_base), -2.0 * jnp.arange(half_dim, dtype=jnp.float32) / HEAD_SIZE)
    angles = token_positions.astype(jnp.float32)[:, None] * inverse[None, :]
    cosine_table = jnp.cos(angles)[:, None, :]
    sine_table = jnp.sin(angles)[:, None, :]
    first_half = shaped[..., :half_dim]
    second_half = shaped[..., half_dim:]
    rotated = jnp.concatenate([first_half * cosine_table - second_half * sine_table, second_half * cosine_table + first_half * sine_table], axis=-1)
    return rotated.astype(jnp.bfloat16)

def key_validity(key_positions, counts):
    key_block = jnp.floor_divide(key_positions, BLOCK_TOKENS)
    within_block = key_positions - key_block * BLOCK_TOKENS
    block_count = counts[jnp.clip(key_block, 0, BLOCKS - 1)]
    return (key_positions >= 0) & (within_block < block_count)

def attend(queries, key_rows_full, value_rows_full, counts):
    span_blocks = WINDOW // BLOCK_TOKENS
    group_length = QUERY_HEAD_COUNT // KEY_VALUE_HEADS
    padding_rows = span_blocks * BLOCK_TOKENS
    key_rows_padded = jnp.concatenate([jnp.zeros((padding_rows, KEY_VALUE_HEADS, HEAD_SIZE), jnp.bfloat16), key_rows_full], axis=0)
    value_rows_padded = jnp.concatenate([jnp.zeros((padding_rows, KEY_VALUE_HEADS, HEAD_SIZE), jnp.bfloat16), value_rows_full], axis=0)
    key_length = (span_blocks + 1) * BLOCK_TOKENS
    scale_factor = 1.0 / math.sqrt(HEAD_SIZE)

    def one_block(block_index):
        first_row = block_index * BLOCK_TOKENS
        block_of_queries = lax.dynamic_slice_in_dim(queries, first_row, BLOCK_TOKENS, 0)
        key_block = lax.dynamic_slice_in_dim(key_rows_padded, first_row, key_length, 0)
        value_block = lax.dynamic_slice_in_dim(value_rows_padded, first_row, key_length, 0)
        query_positions = first_row + jnp.arange(BLOCK_TOKENS, dtype=jnp.int32)
        key_positions = first_row - padding_rows + jnp.arange(key_length, dtype=jnp.int32)
        allowed = key_validity(key_positions, counts)[None, :]
        allowed = allowed & (key_positions[None, :] <= query_positions[:, None])
        allowed = allowed & (query_positions[:, None] - key_positions[None, :] < WINDOW)
        query_broad = block_of_queries.astype(jnp.float32).reshape(BLOCK_TOKENS, KEY_VALUE_HEADS, group_length, HEAD_SIZE)
        key_wide = key_block.astype(jnp.float32)
        scores = jnp.einsum('tkgd,lkd->kgtl', query_broad, key_wide, precision=lax.Precision.HIGHEST) * scale_factor
        scores = jnp.where(allowed[None, None], scores, -jnp.inf)
        largest = lax.optimization_barrier(jnp.max(scores, axis=-1, keepdims=True))
        weights = jnp.exp(scores - largest)
        weights = (weights / lax.optimization_barrier(jnp.sum(weights, axis=-1, keepdims=True))).astype(jnp.bfloat16)
        blended = jnp.einsum('kgtl,lkd->tkgd', weights.astype(jnp.float32), value_block.astype(jnp.float32), precision=lax.Precision.HIGHEST)
        return blended.astype(jnp.bfloat16).reshape(BLOCK_TOKENS, QUERY_HEAD_COUNT * HEAD_SIZE)
    outputs = lax.map(one_block, jnp.arange(BLOCKS, dtype=jnp.int32))
    return outputs.reshape(BLOCKS * BLOCK_TOKENS, QUERY_HEAD_COUNT * HEAD_SIZE)

def reference(tokens, norm_gain, w_query, key_projection_weight, value_projection_weight, w_out, counts):
    hidden = tokens
    token_positions = jnp.arange(SEQUENCE_TOKENS, dtype=jnp.int32)
    group_width = QUERY_HEAD_COUNT * HEAD_SIZE // N_HEAD
    for layer_position in range(LAYER_COUNT):
        normalized_rows = rms_norm(hidden, norm_gain[layer_position])
        queries = apply_rotary_embedding(jnp.dot(normalized_rows, w_query[layer_position], preferred_element_type=jnp.float32), token_positions, QUERY_HEAD_COUNT)
        key_rows_full = apply_rotary_embedding(jnp.dot(normalized_rows, key_projection_weight[layer_position], preferred_element_type=jnp.float32), token_positions, KEY_VALUE_HEADS)
        value_rows_full = jnp.dot(normalized_rows, value_projection_weight[layer_position], preferred_element_type=jnp.float32).astype(jnp.bfloat16).reshape(SEQUENCE_TOKENS, KEY_VALUE_HEADS, HEAD_SIZE)
        attended = attend(queries, key_rows_full, value_rows_full, counts)
        branch = jnp.zeros((SEQUENCE_TOKENS, MODEL_WIDTH), jnp.float32)
        for group_index in range(N_HEAD):
            column_start = group_index * group_width
            partial_product = jnp.dot(attended[:, column_start:column_start + group_width], w_out[layer_position, column_start:column_start + group_width], preferred_element_type=jnp.float32)
            rounded = lax.optimization_barrier(partial_product.astype(jnp.bfloat16))
            branch = branch + rounded.astype(jnp.float32)
        hidden = (hidden.astype(jnp.float32) + branch).astype(jnp.bfloat16)
    return hidden
```

```python
import functools
import math

import jax
import jax.numpy as jnp
from jax import lax
from jax.experimental import pallas as pl
from jax.experimental.pallas import tpu as pltpu
from jax.sharding import PartitionSpec as P

MODEL_WIDTH = 2048
HEAD_SIZE = 128
WINDOW = 4096
LAYER_COUNT = 2
ROWS = 512
HALF = 1024
CHUNK = 128
CHUNKS = 4
SLOTS = 9
NORM_EPSILON = 1e-05
ROPE_BASE = 10000.0
LOW = -1e30
QUERY_SCALE = math.log2(math.e) / math.sqrt(HEAD_SIZE)
NT = (((1,), (1,)), ((), ()))


def mega(
    blocks,
    tok, gain, wq, wk, wv, wo, cos_ref, sin_ref, counts, out_ref,
    xb, wqb, wkvb, wob, nb, qs, kv, vm, m_ref, acc, ab, pb, pr, pb1, pr1,
    ld_sem, ts, tr, zs, zr, xs, xr, os_, or_, cs, cr, ps, pr_sem,
):
    seq = lax.axis_index("seq")
    head = lax.axis_index("head")
    core = lax.rem(seq, 2)
    xlo = lax.rem(lax.div(seq, 2), 2)
    nxt = lax.rem(seq + 4, blocks)
    prv = lax.rem(seq + blocks - 4, blocks)
    xpeer = seq + 2 - 4 * xlo
    cpeer = seq + 1 - 2 * core
    pair = 1 - head
    mesh_id = pl.DeviceIdType.MESH

    def local(src, dst, n):
        return pltpu.make_async_copy(src, dst, ld_sem.at[n])

    loads = [local(tok, xb.at[head], 0)]
    for l in range(LAYER_COUNT):
        loads.append(local(wk.at[l], wkvb.at[l, :, 0:256], 4 * l + 1))
        loads.append(local(wv.at[l], wkvb.at[l, :, 256:512], 4 * l + 2))
        loads.append(local(wq.at[l], wqb.at[l], 4 * l + 3))
        loads.append(local(wo.at[l], wob.at[l], 4 * l + 4))

    barrier = pltpu.get_barrier_semaphore()
    for target in (
        {"seq": prv, "head": head},
        {"seq": xpeer, "head": head},
        {"seq": cpeer, "head": head},
        {"seq": seq, "head": pair},
    ):
        pl.semaphore_signal(barrier, inc=1, device_id=target, device_id_type=mesh_id)
    for load in loads:
        load.start()
    pl.semaphore_wait(barrier, 4)

    def rc_rows(c):
        return pl.ds(c * CHUNK, CHUNK)

    def tok_copy(c):
        return pltpu.make_async_remote_copy(
            src_ref=tok.at[rc_rows(c), :], dst_ref=xb.at[head, rc_rows(c), :],
            send_sem=ts.at[c], recv_sem=tr.at[c],
            device_id={"seq": seq, "head": pair}, device_id_type=mesh_id)

    for c in range(CHUNKS):
        tok_copy(c).start()

    def kv_copy(l, c, src_slot, dst_slot, send, recv, stage, target):
        return pltpu.make_async_remote_copy(
            src_ref=kv.at[l, src_slot, c], dst_ref=kv.at[l, dst_slot, c],
            send_sem=send.at[l, stage, c], recv_sem=recv.at[l, stage, c],
            device_id={"seq": target, "head": head}, device_id_type=mesh_id)

    def z_copy(l, c, i):
        return kv_copy(l, c, 4 * i, 4 * i + 4, zs, zr, i, nxt)

    def x_copy(l, c, i):
        return kv_copy(l, c, 4 * i + 4 * xlo, 4 * i + 2, xs, xr, i, xpeer)

    def o_copy(l, c, i):
        return kv_copy(l, c, 4 * i + 4 * core, 4 * i + 1 + 2 * core, os_, or_, i, cpeer)

    def c_copy(l, c, i):
        return kv_copy(l, c, 4 * i + 2, 4 * i + 3 - 2 * core, cs, cr, i, cpeer)

    def event0(l, c):
        z_copy(l, c, 0).start()

        @pl.when(xlo == 0)
        def _():
            x_copy(l, c, 0).start()

        @pl.when(core == 0)
        def _():
            o_copy(l, c, 0).start()

    def event1(l, c):
        z_copy(l, c, 0).wait_recv()
        z_copy(l, c, 1).start()

        @pl.when(xlo == 1)
        def _():
            x_copy(l, c, 0).start()

        @pl.when(xlo == 0)
        def _():
            x_copy(l, c, 1).start()

        @pl.when(core == 1)
        def _():
            o_copy(l, c, 0).start()

        @pl.when(core == 0)
        def _():
            o_copy(l, c, 1).start()

    def event2(l, c):
        x_copy(l, c, 0).wait_recv()
        c_copy(l, c, 0).start()

    def event3(l, c):
        z_copy(l, c, 1).wait_recv()

        @pl.when(xlo == 1)
        def _():
            x_copy(l, c, 1).start()

        @pl.when(core == 1)
        def _():
            o_copy(l, c, 1).start()

    def event4(l, c):
        x_copy(l, c, 1).wait_recv()
        c_copy(l, c, 1).start()

    own_count = counts[seq]
    lanes = lax.broadcasted_iota(jnp.int32, (16, ROWS), 1)
    sub = lax.broadcasted_iota(jnp.int32, (16, ROWS), 0)
    for d in range(SLOTS):
        n_valid = counts[lax.rem(seq + blocks - d, blocks)]
        vm[d] = jnp.where((lanes < n_valid) & (sub == 0), 1.0, 0.0).astype(jnp.bfloat16)
    far_count = counts[lax.rem(seq + blocks - 8, blocks)]

    def rope(val, cos, sin):
        return val * cos + pltpu.roll(val, 64, 1) * sin

    def project(l, c):
        rows = rc_rows(c)
        x0 = xb[0, rows, :].astype(jnp.float32)
        x1 = xb[1, rows, :].astype(jnp.float32)
        total = jnp.sum(x0 * x0, axis=1, keepdims=True) + jnp.sum(x1 * x1, axis=1, keepdims=True)
        factor = lax.rsqrt(total / MODEL_WIDTH + NORM_EPSILON)
        nb[:, 0:HALF] = (x0 * factor * gain[l : l + 1, 0:HALF]).astype(jnp.bfloat16)
        nb[:, HALF:] = (x1 * factor * gain[l : l + 1, HALF:]).astype(jnp.bfloat16)
        cos = cos_ref[rows, :]
        sin = sin_ref[rows, :]
        kvp = jnp.dot(nb[...], wkvb[l], preferred_element_type=jnp.float32)
        valid = lax.broadcasted_iota(jnp.int32, (CHUNK, HEAD_SIZE), 0) + c * CHUNK < own_count
        for g in range(2):
            key = rope(kvp[:, g * 128 : (g + 1) * 128], cos, sin).astype(jnp.bfloat16)
            if c > 0:
                first = kv[l, 0, 0, g * 128 : g * 128 + 1, :]
                key = jnp.where(valid, key.astype(jnp.float32), first.astype(jnp.float32)).astype(jnp.bfloat16)
            kv[l, 0, c, g * 128 : (g + 1) * 128, :] = key
            val = jnp.where(valid, kvp[:, 256 + g * 128 : 256 + (g + 1) * 128], 0.0)
            kv[l, 0, c, 256 + g * 128 : 256 + (g + 1) * 128, :] = val.T.astype(jnp.bfloat16)
        event0(l, c)
        for half in range(2):
            qp = jnp.dot(nb[...], wqb[l, :, half * 512 : (half + 1) * 512], preferred_element_type=jnp.float32)
            for h in range(4):
                rot = rope(qp[:, h * 128 : (h + 1) * 128], cos, sin) * QUERY_SCALE
                qs[half * 4 + c, h * 128 : (h + 1) * 128, :] = rot.astype(jnp.bfloat16)

    def keys_of(l, slot, g, lo, hi):
        return jnp.concatenate([kv[l, slot, c, g * 128 : (g + 1) * 128, :] for c in range(lo, hi)], axis=0)

    def values_of(l, slot, g, lo, hi):
        vt = jnp.concatenate([kv[l, slot, c, 256 + g * 128 : 256 + (g + 1) * 128, :] for c in range(lo, hi)], axis=1)
        return jnp.concatenate([vt, vm[slot, :, lo * 128 : hi * 128]], axis=0)

    units = [(g, c) for g in range(2) for c in range(CHUNKS)]

    def scores(l, slot, g, c, lo, hi):
        return lax.dot_general(keys_of(l, slot, g, lo, hi), qs[g * 4 + c], NT, preferred_element_type=jnp.float32)

    def sweep(l, slot, bounds, mask, first):
        nxt_s = scores(l, slot, *units[0], *bounds(units[0][1]))
        for n, (g, c) in enumerate(units):
            s = nxt_s
            if n + 1 < len(units):
                nxt_s = scores(l, slot, *units[n + 1], *bounds(units[n + 1][1]))
            lo, hi = bounds(c)
            u = g * 4 + c
            if mask is not None:
                key_at = lax.broadcasted_iota(jnp.int32, s.shape, 0) + lo * 128
                row_at = (lax.broadcasted_iota(jnp.int32, s.shape, 1) & 127) + c * CHUNK
                s = jnp.where(mask(key_at, row_at), s, LOW)
            top = jnp.max(s, axis=0, keepdims=True)
            if first:
                m_new = top
            else:
                m_old = m_ref[u]
                m_new = jnp.maximum(m_old, top)
            p = jnp.exp2(s - m_new).astype(jnp.bfloat16)
            part = jnp.dot(values_of(l, slot, g, lo, hi), p, preferred_element_type=jnp.float32)
            m_ref[u] = m_new
            if first:
                acc[u] = part
            else:
                acc[u] = acc[u] * jnp.exp2(m_old - m_new) + part

    def attention(l):
        sweep(l, 0, lambda c: (0, c + 1), lambda key_at, row_at: key_at <= row_at, True)
        event1(l, 3)
        event2(l, 2)
        event3(l, 2)
        event4(l, 1)

        def step(n, carry):
            @pl.when(n == 1)
            def _():
                event2(l, 3)
                event3(l, 3)
                event4(l, 2)
                for c in range(CHUNKS):
                    o_copy(l, c, 0).wait_recv()

            @pl.when(n == 3)
            def _():
                event4(l, 3)
                for c in range(CHUNKS):
                    c_copy(l, c, 0).wait_recv()

                @pl.when(seq >= 8)
                def _():
                    sweep(l, 8, lambda c: (c, 4), lambda key_at, row_at: (key_at > row_at) & (key_at < far_count), False)

            @pl.when(n == 5)
            def _():
                for c in range(CHUNKS):
                    o_copy(l, c, 1).wait_recv()

            @pl.when(n == 6)
            def _():
                for c in range(CHUNKS):
                    c_copy(l, c, 1).wait_recv()

            sub_n = n % 4
            base = 4 * (n // 4)
            slot_lo = jnp.where(
                n == 0, 4, jnp.where(
                    n == 1, 3 - 2 * core, jnp.where(
                        n == 2, 2, jnp.where(
                            n == 3, 1 + 2 * core, jnp.where(
                                n == 4, 6, jnp.where(n == 5, 7 - 2 * core, 5 + 2 * core))))))

            @pl.when(seq >= slot_lo)
            def _():
                sweep(l, slot_lo, lambda c: (0, 4), None, False)

            return carry

        lax.fori_loop(0, 7, step, 0)

    def attended(c):
        for g in range(2):
            u = g * 4 + c
            norm = acc[u, 0:128, :] / acc[u, 128:129, :]
            for h in range(4):
                ab[:, (g * 4 + h) * 128 : (g * 4 + h + 1) * 128] = norm[:, h * 128 : (h + 1) * 128].T.astype(jnp.bfloat16)

    def full_copy(c):
        return pltpu.make_async_remote_copy(
            src_ref=pb.at[c], dst_ref=pr.at[c], send_sem=ps.at[0, c], recv_sem=pr_sem.at[0, c],
            device_id={"seq": seq, "head": pair}, device_id_type=mesh_id)

    def half_copy(c):
        return pltpu.make_async_remote_copy(
            src_ref=pb1.at[c], dst_ref=pr1.at[c], send_sem=ps.at[1, c], recv_sem=pr_sem.at[1, c],
            device_id={"seq": seq, "head": pair}, device_id_type=mesh_id)

    def early_events(l, c):
        if c >= 1:
            event1(l, c - 1)
        if c >= 2:
            event2(l, c - 2)
            event3(l, c - 2)
        if c >= 3:
            event4(l, c - 3)

    loads[0].wait()
    for c in range(CHUNKS):
        tok_copy(c).wait_recv()
        if c == 0:
            for load in loads[1:4]:
                load.wait()
        project(0, c)
        early_events(0, c)
    attention(0)
    loads[4].wait()
    for c in range(CHUNKS):
        attended(c)
        for half in range(2):
            pb[c, :, half * HALF : (half + 1) * HALF] = jnp.dot(
                ab[...], wob[0, :, half * HALF : (half + 1) * HALF], preferred_element_type=jnp.float32
            ).astype(jnp.bfloat16)
        full_copy(c).start()

    for load in loads[5:8]:
        load.wait()
    for c in range(CHUNKS):
        full_copy(c).wait_recv()
        rows = rc_rows(c)
        for half in range(2):
            cols = slice(half * HALF, (half + 1) * HALF)
            summed = pb[c, :, cols].astype(jnp.float32) + pr[c, :, cols].astype(jnp.float32)
            xb[half, rows, :] = (xb[half, rows, :].astype(jnp.float32) + summed).astype(jnp.bfloat16)
        project(1, c)
        early_events(1, c)
    attention(1)
    loads[8].wait()
    other_cols = pl.ds(pl.multiple_of(pair * HALF, HALF), HALF)
    own_cols = pl.ds(pl.multiple_of(head * HALF, HALF), HALF)
    for c in range(CHUNKS):
        rows = rc_rows(c)
        attended(c)
        pb1[c] = jnp.dot(ab[...], wob[1, :, other_cols], preferred_element_type=jnp.float32).astype(jnp.bfloat16)
        half_copy(c).start()
        out_ref[rows, :] = jnp.dot(ab[...], wob[1, :, own_cols], preferred_element_type=jnp.float32).astype(jnp.bfloat16)
    for c in range(CHUNKS):
        rows = rc_rows(c)
        half_copy(c).wait_recv()
        summed = out_ref[rows, :].astype(jnp.float32) + pr1[c].astype(jnp.float32)
        out_ref[rows, :] = (xb[head, rows, :].astype(jnp.float32) + summed).astype(jnp.bfloat16)

    for c in range(CHUNKS):
        tok_copy(c).wait_send()
        full_copy(c).wait_send()
        half_copy(c).wait_send()
        for l in range(LAYER_COUNT):
            for i in range(2):
                z_copy(l, c, i).wait_send()
                x_copy(l, c, i).wait_send()
                o_copy(l, c, i).wait_send()
                c_copy(l, c, i).wait_send()


def per_device(tokens, norm_gain, w_query, key_projection_weight, value_projection_weight, w_out, counts):
    blocks = lax.axis_size("seq")
    half_dim = HEAD_SIZE // 2
    positions = lax.axis_index("seq") * ROWS + jnp.arange(ROWS, dtype=jnp.int32)
    inverse = jnp.power(jnp.float32(ROPE_BASE), -2.0 * jnp.arange(half_dim, dtype=jnp.float32) / HEAD_SIZE)
    angles = positions.astype(jnp.float32)[:, None] * inverse[None, :]
    cosine, sine = jnp.cos(angles), jnp.sin(angles)
    cos2 = jnp.concatenate([cosine, cosine], axis=1)
    sin2 = jnp.concatenate([-sine, sine], axis=1)
    bf16, f32 = jnp.bfloat16, jnp.float32
    any_, vmem = pl.BlockSpec(memory_space=pl.ANY), pl.BlockSpec(memory_space=pltpu.VMEM)
    dma = pltpu.SemaphoreType.DMA
    return pl.pallas_call(
        functools.partial(mega, blocks),
        out_shape=jax.ShapeDtypeStruct((ROWS, HALF), bf16),
        in_specs=[any_, vmem, any_, any_, any_, any_, vmem, vmem, pl.BlockSpec(memory_space=pltpu.SMEM)],
        out_specs=vmem,
        scratch_shapes=[
            pltpu.VMEM((2, ROWS, HALF), bf16),
            pltpu.VMEM((2, MODEL_WIDTH, HALF), bf16),
            pltpu.VMEM((2, MODEL_WIDTH, 512), bf16),
            pltpu.VMEM((2, HALF, MODEL_WIDTH), bf16),
            pltpu.VMEM((CHUNK, MODEL_WIDTH), bf16),
            pltpu.VMEM((8, 512, 128), bf16),
            pltpu.VMEM((2, SLOTS, CHUNKS, 512, 128), bf16),
            pltpu.VMEM((SLOTS, 16, ROWS), bf16),
            pltpu.VMEM((8, 1, 512), f32),
            pltpu.VMEM((8, 144, 512), f32),
            pltpu.VMEM((CHUNK, HALF), bf16),
            pltpu.VMEM((CHUNKS, CHUNK, MODEL_WIDTH), bf16),
            pltpu.VMEM((CHUNKS, CHUNK, MODEL_WIDTH), bf16),
            pltpu.VMEM((CHUNKS, CHUNK, HALF), bf16),
            pltpu.VMEM((CHUNKS, CHUNK, HALF), bf16),
            dma((9,)), dma((4,)), dma((4,)),
            dma((2, 2, 4)), dma((2, 2, 4)), dma((2, 2, 4)), dma((2, 2, 4)),
            dma((2, 2, 4)), dma((2, 2, 4)), dma((2, 2, 4)), dma((2, 2, 4)),
            dma((2, 4)), dma((2, 4)),
        ],
        compiler_params=pltpu.CompilerParams(
            collective_id=0, has_side_effects=True, vmem_limit_bytes=63 * 2**20
        ),
    )(tokens, norm_gain, w_query, key_projection_weight, value_projection_weight, w_out, cos2, sin2, counts)


def solution(mesh):
    return jax.shard_map(
        per_device,
        mesh=mesh,
        in_specs=(
            P("seq", "head"),
            P(),
            P(None, None, "head"),
            P(None, None, "head"),
            P(None, None, "head"),
            P(None, "head", None),
            P(),
        ),
        out_specs=P("seq", "head"),
        check_vma=False,
    )
```

```python
import functools
import math

import jax
import jax.numpy as jnp
import numpy as np
from jax import lax
from jax.experimental import pallas as pl
from jax.experimental.pallas import tpu as pltpu
from jax.sharding import PartitionSpec as P

MODEL_WIDTH = 2048
HEAD_SIZE = 128
WINDOW = 4096
LAYER_COUNT = 2
ROWS = 512
HALF = 1024
CHUNK = 128
CHUNKS = 4
SLOTS = 9
NORM_EPSILON = 1e-05
ROPE_BASE = 10000.0
LOW = -1e30
QUERY_SCALE = math.log2(math.e) / math.sqrt(HEAD_SIZE)
NT = (((1,), (1,)), ((), ()))


def mega(
    blocks,
    tok, gain, wq, wk, wv, wo, cos_tab, sin_tab, counts, out_ref,
    cos_ref, sin_ref, xb, wqb, wkvb, wob, nb, qs, kv, vm, m_ref, acc, ab, pb, pr, pb1, pr1,
    ld_sem, ts, tr, zs, zr, xs, xr, os_, or_, cs, cr, ps, pr_sem,
):
    seq = lax.axis_index("seq")
    head = lax.axis_index("head")
    core = lax.rem(seq, 2)
    xlo = lax.rem(lax.div(seq, 2), 2)
    nxt = lax.rem(seq + 4, blocks)
    prv = lax.rem(seq + blocks - 4, blocks)
    xpeer = seq + 2 - 4 * xlo
    cpeer = seq + 1 - 2 * core
    pair = 1 - head
    mesh_id = pl.DeviceIdType.MESH

    def local(src, dst, n):
        return pltpu.make_async_copy(src, dst, ld_sem.at[n])

    loads = [local(tok, xb.at[head], 0)]
    for l in range(LAYER_COUNT):
        loads.append(local(wk.at[l], wkvb.at[l, :, 0:256], 4 * l + 1))
        loads.append(local(wv.at[l], wkvb.at[l, :, 256:512], 4 * l + 2))
        loads.append(local(wq.at[l], wqb.at[l], 4 * l + 3))
        loads.append(local(wo.at[l], wob.at[l], 4 * l + 4))

    barrier = pltpu.get_barrier_semaphore()
    for target in (
        {"seq": prv, "head": head},
        {"seq": xpeer, "head": head},
        {"seq": cpeer, "head": head},
        {"seq": seq, "head": pair},
    ):
        pl.semaphore_signal(barrier, inc=1, device_id=target, device_id_type=mesh_id)
    for load in loads:
        load.start()
    pl.semaphore_wait(barrier, 4)

    def rc_rows(c):
        return pl.ds(c * CHUNK, CHUNK)

    def tok_copy(c):
        return pltpu.make_async_remote_copy(
            src_ref=tok.at[rc_rows(c), :], dst_ref=xb.at[head, rc_rows(c), :],
            send_sem=ts.at[c], recv_sem=tr.at[c],
            device_id={"seq": seq, "head": pair}, device_id_type=mesh_id)

    for c in range(CHUNKS):
        tok_copy(c).start()

    def kv_copy(l, c, src_slot, dst_slot, send, recv, stage, target):
        return pltpu.make_async_remote_copy(
            src_ref=kv.at[l, src_slot, c], dst_ref=kv.at[l, dst_slot, c],
            send_sem=send.at[l, stage, c], recv_sem=recv.at[l, stage, c],
            device_id={"seq": target, "head": head}, device_id_type=mesh_id)

    def z_copy(l, c, i):
        return kv_copy(l, c, 4 * i, 4 * i + 4, zs, zr, i, nxt)

    def x_copy(l, c, i):
        return kv_copy(l, c, 4 * i + 4 * xlo, 4 * i + 2, xs, xr, i, xpeer)

    def o_copy(l, c, i):
        return kv_copy(l, c, 4 * i + 4 * core, 4 * i + 1 + 2 * core, os_, or_, i, cpeer)

    def c_copy(l, c, i):
        return kv_copy(l, c, 4 * i + 2, 4 * i + 3 - 2 * core, cs, cr, i, cpeer)

    def event0(l, c):
        z_copy(l, c, 0).start()

        @pl.when(xlo == 0)
        def _():
            x_copy(l, c, 0).start()

        @pl.when(core == 0)
        def _():
            o_copy(l, c, 0).start()

    def event1(l, c):
        z_copy(l, c, 0).wait_recv()
        z_copy(l, c, 1).start()

        @pl.when(xlo == 1)
        def _():
            x_copy(l, c, 0).start()

        @pl.when(xlo == 0)
        def _():
            x_copy(l, c, 1).start()

        @pl.when(core == 1)
        def _():
            o_copy(l, c, 0).start()

        @pl.when(core == 0)
        def _():
            o_copy(l, c, 1).start()

    def event2(l, c):
        x_copy(l, c, 0).wait_recv()
        c_copy(l, c, 0).start()

    def event3(l, c):
        z_copy(l, c, 1).wait_recv()

        @pl.when(xlo == 1)
        def _():
            x_copy(l, c, 1).start()

        @pl.when(core == 1)
        def _():
            o_copy(l, c, 1).start()

    def event4(l, c):
        x_copy(l, c, 1).wait_recv()
        c_copy(l, c, 1).start()

    cb, sb = cos_tab[pl.ds(seq, 1), :], sin_tab[pl.ds(seq, 1), :]
    ci, si = cos_tab[64:80, :], sin_tab[64:80, :]
    run_cos, run_sin = cb * ci - sb * si, sb * ci + cb * si
    cj, sj = cos_tab[80:112, :], sin_tab[80:112, :]
    sign = jnp.where(lax.broadcasted_iota(jnp.int32, (32, HEAD_SIZE), 1) < 64, -1.0, 1.0)
    for i in range(16):
        a, b = run_cos[i : i + 1, :], run_sin[i : i + 1, :]
        cos_ref[i * 32 : (i + 1) * 32, :] = a * cj - b * sj
        sin_ref[i * 32 : (i + 1) * 32, :] = (b * cj + a * sj) * sign

    own_count = counts[seq]
    lanes = lax.broadcasted_iota(jnp.int32, (16, ROWS), 1)
    sub = lax.broadcasted_iota(jnp.int32, (16, ROWS), 0)
    for d in range(SLOTS):
        n_valid = counts[lax.rem(seq + blocks - d, blocks)]
        vm[d] = jnp.where((lanes < n_valid) & (sub == 0), 1.0, 0.0).astype(jnp.bfloat16)
    far_count = counts[lax.rem(seq + blocks - 8, blocks)]

    def rope(val, cos, sin):
        return val * cos + pltpu.roll(val, 64, 1) * sin

    def project(l, c):
        rows = rc_rows(c)
        x0 = xb[0, rows, :].astype(jnp.float32)
        x1 = xb[1, rows, :].astype(jnp.float32)
        total = jnp.sum(x0 * x0, axis=1, keepdims=True) + jnp.sum(x1 * x1, axis=1, keepdims=True)
        factor = lax.rsqrt(total / MODEL_WIDTH + NORM_EPSILON)
        nb[:, 0:HALF] = (x0 * factor * gain[pl.ds(l, 1), 0:HALF]).astype(jnp.bfloat16)
        nb[:, HALF:] = (x1 * factor * gain[pl.ds(l, 1), HALF:]).astype(jnp.bfloat16)
        cos = cos_ref[rows, :]
        sin = sin_ref[rows, :]
        kvp = jnp.dot(nb[...], wkvb[l], preferred_element_type=jnp.float32)
        valid = lax.broadcasted_iota(jnp.int32, (CHUNK, HEAD_SIZE), 0) + c * CHUNK < own_count
        for g in range(2):
            key = rope(kvp[:, g * 128 : (g + 1) * 128], cos, sin).astype(jnp.bfloat16)
            if c > 0:
                first = kv[l, 0, 0, g * 128 : g * 128 + 1, :]
                key = jnp.where(valid, key.astype(jnp.float32), first.astype(jnp.float32)).astype(jnp.bfloat16)
            kv[l, 0, c, g * 128 : (g + 1) * 128, :] = key
            val = jnp.where(valid, kvp[:, 256 + g * 128 : 256 + (g + 1) * 128], 0.0)
            kv[l, 0, c, 256 + g * 128 : 256 + (g + 1) * 128, :] = val.T.astype(jnp.bfloat16)
        event0(l, c)
        for half in range(2):
            qp = jnp.dot(nb[...], wqb[l, :, half * 512 : (half + 1) * 512], preferred_element_type=jnp.float32)
            for h in range(4):
                rot = rope(qp[:, h * 128 : (h + 1) * 128], cos, sin) * QUERY_SCALE
                qs[half * 4 + c, h * 128 : (h + 1) * 128, :] = rot.astype(jnp.bfloat16)

    def keys_of(l, slot, g, lo, hi):
        return jnp.concatenate([kv[l, slot, c, g * 128 : (g + 1) * 128, :] for c in range(lo, hi)], axis=0)

    def values_of(l, slot, g, lo, hi):
        vt = jnp.concatenate([kv[l, slot, c, 256 + g * 128 : 256 + (g + 1) * 128, :] for c in range(lo, hi)], axis=1)
        return jnp.concatenate([vt, vm[slot, :, lo * 128 : hi * 128]], axis=0)

    def fold(l, slot, g, c, lo, hi, s, mask, first):
        u = g * 4 + c
        if mask is not None:
            key_at = lax.broadcasted_iota(jnp.int32, s.shape, 0) + lo * 128
            row_at = (lax.broadcasted_iota(jnp.int32, s.shape, 1) & 127) + c * CHUNK
            s = jnp.where(mask(key_at, row_at), s, LOW)
        top = jnp.max(s, axis=0, keepdims=True)
        if first:
            m_new = top
        else:
            m_old = m_ref[u]
            m_new = jnp.maximum(m_old, top)
        p = jnp.exp2(s - m_new).astype(jnp.bfloat16)
        part = jnp.dot(values_of(l, slot, g, lo, hi), p, preferred_element_type=jnp.float32)
        m_ref[u] = m_new
        if first:
            acc[u] = part
        else:
            acc[u] = acc[u] * jnp.exp2(m_old - m_new) + part

    def scores(l, slot, g, c, lo, hi):
        return lax.dot_general(keys_of(l, slot, g, lo, hi), qs[g * 4 + c], NT, preferred_element_type=jnp.float32)

    def sweep(l, tiles, mask=None, first=False):
        nxt_s = scores(l, *tiles[0])
        for n, tile in enumerate(tiles):
            s = nxt_s
            if n + 1 < len(tiles):
                nxt_s = scores(l, *tiles[n + 1])
            fold(l, *tile, s, mask, first)

    def attention(l):
        every = [(g, c) for g in range(2) for c in range(CHUNKS)]
        sweep(l, [(0, g, c, 0, c + 1) for g, c in every], lambda key_at, row_at: key_at <= row_at, True)
        event1(l, 3)
        event2(l, 2)
        event3(l, 2)
        event4(l, 1)
        event2(l, 3)
        event3(l, 3)

        @pl.when(seq >= 8)
        def _():
            sweep(l, [(8, g, c, c, 4) for g, c in every], lambda key_at, row_at: (key_at > row_at) & (key_at < far_count))

        event4(l, 2)
        event4(l, 3)
        for c in range(CHUNKS):
            o_copy(l, c, 0).wait_recv()
            c_copy(l, c, 0).wait_recv()
            o_copy(l, c, 1).wait_recv()
            c_copy(l, c, 1).wait_recv()

    def middle(l, c):
        @pl.when(seq >= 8)
        def _():
            sweep(l, [(slot, g, c, 0, 4) for slot in range(1, 8) for g in range(2)])

        @pl.when(seq < 8)
        def _():
            def one(slot, carry):
                sweep(l, [(slot, g, c, 0, 4) for g in range(2)])
                return carry

            lax.fori_loop(1, jnp.minimum(seq + 1, 8), one, 0)

    def attended(c):
        for g in range(2):
            u = g * 4 + c
            norm = acc[u, 0:128, :] / acc[u, 128:129, :]
            for h in range(4):
                ab[:, (g * 4 + h) * 128 : (g * 4 + h + 1) * 128] = norm[:, h * 128 : (h + 1) * 128].T.astype(jnp.bfloat16)

    def full_copy(c):
        return pltpu.make_async_remote_copy(
            src_ref=pb.at[c], dst_ref=pr.at[c], send_sem=ps.at[0, c], recv_sem=pr_sem.at[0, c],
            device_id={"seq": seq, "head": pair}, device_id_type=mesh_id)

    def half_copy(c):
        return pltpu.make_async_remote_copy(
            src_ref=pb1.at[c], dst_ref=pr1.at[c], send_sem=ps.at[1, c], recv_sem=pr_sem.at[1, c],
            device_id={"seq": seq, "head": pair}, device_id_type=mesh_id)

    def early_events(l, c):
        if c >= 1:
            event1(l, c - 1)
        if c >= 2:
            event2(l, c - 2)
            event3(l, c - 2)
        if c >= 3:
            event4(l, c - 3)

    other_cols = pl.ds(pl.multiple_of(pair * HALF, HALF), HALF)
    own_cols = pl.ds(pl.multiple_of(head * HALF, HALF), HALF)

    def dots(l, cols):
        return jnp.dot(ab[...], wob[l, :, cols], preferred_element_type=jnp.float32).astype(jnp.bfloat16)

    def layer(l, carry):
        for c in range(CHUNKS):
            rows = rc_rows(c)

            @pl.when(l == 0)
            def _():
                if c == 0:
                    for load in loads[0:4]:
                        load.wait()
                tok_copy(c).wait_recv()

            @pl.when(l == 1)
            def _():
                if c == 0:
                    for load in loads[5:8]:
                        load.wait()
                full_copy(c).wait_recv()
                for half in range(2):
                    cols = slice(half * HALF, (half + 1) * HALF)
                    summed = pb[c, :, cols].astype(jnp.float32) + pr[c, :, cols].astype(jnp.float32)
                    xb[half, rows, :] = (xb[half, rows, :].astype(jnp.float32) + summed).astype(jnp.bfloat16)

            project(l, c)
            early_events(l, c)
        attention(l)

        @pl.when(l == 0)
        def _():
            loads[4].wait()

        @pl.when(l == 1)
        def _():
            loads[8].wait()

        def chunk(c, carry):
            rows = pl.ds(pl.multiple_of(c * CHUNK, CHUNK), CHUNK)
            middle(l, c)
            attended(c)

            @pl.when(l == 0)
            def _():
                for half in range(2):
                    pb[c, :, half * HALF : (half + 1) * HALF] = dots(0, pl.ds(half * HALF, HALF))
                full_copy(c).start()

            @pl.when(l == 1)
            def _():
                pb1[c] = dots(1, other_cols)
                half_copy(c).start()
                out_ref[rows, :] = dots(1, own_cols)

            return carry

        return lax.fori_loop(0, CHUNKS, chunk, carry)

    lax.fori_loop(0, LAYER_COUNT, layer, 0)
    for c in range(CHUNKS):
        rows = rc_rows(c)
        half_copy(c).wait_recv()
        summed = out_ref[rows, :].astype(jnp.float32) + pr1[c].astype(jnp.float32)
        out_ref[rows, :] = (xb[head, rows, :].astype(jnp.float32) + summed).astype(jnp.bfloat16)

    for c in range(CHUNKS):
        tok_copy(c).wait_send()
        full_copy(c).wait_send()
        half_copy(c).wait_send()
        for l in range(LAYER_COUNT):
            for i in range(2):
                z_copy(l, c, i).wait_send()
                x_copy(l, c, i).wait_send()
                o_copy(l, c, i).wait_send()
                c_copy(l, c, i).wait_send()


def per_device(tokens, norm_gain, w_query, key_projection_weight, value_projection_weight, w_out, counts):
    blocks = lax.axis_size("seq")
    half_dim = HEAD_SIZE // 2
    inverse = ROPE_BASE ** (-2.0 * np.arange(half_dim) / HEAD_SIZE)
    offsets = np.concatenate([np.arange(64) * ROWS, np.arange(16) * 32, np.arange(32)])
    angles = np.tile(offsets[:, None] * inverse[None, :], (1, 2))
    cos2 = jnp.asarray(np.cos(angles), jnp.float32)
    sin2 = jnp.asarray(np.sin(angles), jnp.float32)
    bf16, f32 = jnp.bfloat16, jnp.float32
    any_, vmem = pl.BlockSpec(memory_space=pl.ANY), pl.BlockSpec(memory_space=pltpu.VMEM)
    dma = pltpu.SemaphoreType.DMA
    return pl.pallas_call(
        functools.partial(mega, blocks),
        out_shape=jax.ShapeDtypeStruct((ROWS, HALF), bf16),
        in_specs=[any_, vmem, any_, any_, any_, any_, vmem, vmem, pl.BlockSpec(memory_space=pltpu.SMEM)],
        out_specs=vmem,
        scratch_shapes=[
            pltpu.VMEM((ROWS, HEAD_SIZE), f32),
            pltpu.VMEM((ROWS, HEAD_SIZE), f32),
            pltpu.VMEM((2, ROWS, HALF), bf16),
            pltpu.VMEM((2, MODEL_WIDTH, HALF), bf16),
            pltpu.VMEM((2, MODEL_WIDTH, 512), bf16),
            pltpu.VMEM((2, HALF, MODEL_WIDTH), bf16),
            pltpu.VMEM((CHUNK, MODEL_WIDTH), bf16),
            pltpu.VMEM((8, 512, 128), bf16),
            pltpu.VMEM((2, SLOTS, CHUNKS, 512, 128), bf16),
            pltpu.VMEM((SLOTS, 16, ROWS), bf16),
            pltpu.VMEM((8, 1, 512), f32),
            pltpu.VMEM((8, 144, 512), f32),
            pltpu.VMEM((CHUNK, HALF), bf16),
            pltpu.VMEM((CHUNKS, CHUNK, MODEL_WIDTH), bf16),
            pltpu.VMEM((CHUNKS, CHUNK, MODEL_WIDTH), bf16),
            pltpu.VMEM((CHUNKS, CHUNK, HALF), bf16),
            pltpu.VMEM((CHUNKS, CHUNK, HALF), bf16),
            dma((9,)), dma((4,)), dma((4,)),
            dma((2, 2, 4)), dma((2, 2, 4)), dma((2, 2, 4)), dma((2, 2, 4)),
            dma((2, 2, 4)), dma((2, 2, 4)), dma((2, 2, 4)), dma((2, 2, 4)),
            dma((2, 4)), dma((2, 4)),
        ],
        compiler_params=pltpu.CompilerParams(
            collective_id=0, has_side_effects=True, vmem_limit_bytes=63 * 2**20
        ),
    )(tokens, norm_gain, w_query, key_projection_weight, value_projection_weight, w_out, cos2, sin2, counts)


def solution(mesh):
    return jax.shard_map(
        per_device,
        mesh=mesh,
        in_specs=(
            P("seq", "head"),
            P(),
            P(None, None, "head"),
            P(None, None, "head"),
            P(None, None, "head"),
            P(None, "head", None),
            P(),
        ),
        out_specs=P("seq", "head"),
        check_vma=False,
    )
```

```python
import functools
import math

import jax
import jax.numpy as jnp
import numpy as np
from jax import lax
from jax.experimental import pallas as pl
from jax.experimental.pallas import tpu as pltpu
from jax.sharding import PartitionSpec as P

MODEL_WIDTH = 2048
HEAD_SIZE = 128
WINDOW = 4096
LAYER_COUNT = 2
ROWS = 512
HALF = 1024
CHUNK = 128
CHUNKS = 4
SLOTS = 9
NORM_EPSILON = 1e-05
ROPE_BASE = 10000.0
LOW = -1e30
QUERY_SCALE = math.log2(math.e) / math.sqrt(HEAD_SIZE)
NT = (((1,), (1,)), ((), ()))


def mega(
    blocks,
    tok, gain, wq, wk, wv, wo, cos_tab, sin_tab, counts, out_ref,
    cos_ref, sin_ref, xb, wqb, wkvb, wob, nb, qs, kv, vm, m_ref, acc, pbuf, ab, pb, pr, pb1, pr1, wot,
    ld_sem, ts, tr, zs, zr, xs, xr, os_, or_, cs, cr, ps, pr_sem, ws, wr,
):
    seq = lax.axis_index("seq")
    head = lax.axis_index("head")
    core = lax.rem(seq, 2)
    xlo = lax.rem(lax.div(seq, 2), 2)
    nxt = lax.rem(seq + 4, blocks)
    prv = lax.rem(seq + blocks - 4, blocks)
    xpeer = seq + 2 - 4 * xlo
    cpeer = seq + 1 - 2 * core
    pair = 1 - head
    zi = lax.rem(lax.div(seq, 4), 4)
    yi = lax.div(seq, 16)

    def z_peer(k):
        return seq + 4 * (lax.rem(zi + k, 4) - zi)

    def y_peer(k):
        return seq + 16 * (lax.rem(yi + k, 4) - yi)

    mesh_id = pl.DeviceIdType.MESH

    def local(src, dst, n):
        return pltpu.make_async_copy(src, dst, ld_sem.at[n])

    loads = [local(tok, xb.at[head], 0)]
    for l in range(LAYER_COUNT):
        loads.append(local(wk.at[l], wkvb.at[l, :, 0:256], 4 * l + 1))
        loads.append(local(wv.at[l], wkvb.at[l, :, 256:512], 4 * l + 2))
        loads.append(local(wq.at[l], wqb.at[l], 4 * l + 3))
        loads.append(local(wo.at[l], wob.at[l], 4 * l + 4))

    barrier = pltpu.get_barrier_semaphore()
    for target in (
        {"seq": prv, "head": head},
        {"seq": xpeer, "head": head},
        {"seq": cpeer, "head": head},
        {"seq": seq, "head": pair},
        *({"seq": z_peer(k), "head": head} for k in (1, 2, 3)),
        *({"seq": y_peer(k), "head": head} for k in (1, 2, 3)),
    ):
        pl.semaphore_signal(barrier, inc=1, device_id=target, device_id_type=mesh_id)
    for load in loads:
        load.start()
    pl.semaphore_wait(barrier, 10)

    def rc_rows(c):
        return pl.ds(c * CHUNK, CHUNK)

    def tok_copy(c):
        return pltpu.make_async_remote_copy(
            src_ref=tok.at[rc_rows(c), :], dst_ref=xb.at[head, rc_rows(c), :],
            send_sem=ts.at[c], recv_sem=tr.at[c],
            device_id={"seq": seq, "head": pair}, device_id_type=mesh_id)

    def w_copy(src, base, rows, n, target, other_head=False):
        at = pl.ds(pl.multiple_of(base, 16), rows)
        return pltpu.make_async_remote_copy(
            src_ref=src.at[at, :], dst_ref=wot.at[at, :], send_sem=ws.at[n], recv_sem=wr.at[n],
            device_id={"seq": target, "head": pair if other_head else head}, device_id_type=mesh_id)

    w_base = (core * 512, core * 512 + 256)
    w_piece = (w_base[0] + (zi * 4 + yi) * 16, w_base[1] + (yi * 4 + zi) * 16)
    w_group = (w_base[0] + zi * 64, w_base[1] + yi * 64)

    def w_pair(o):
        return w_copy(wo.at[0], w_piece[o], 16, o, seq, True)

    def w_small(o, k):
        return w_copy(wot, w_piece[o], 16, 2 + 3 * o + k - 1, (y_peer, z_peer)[o](k))

    def w_big(o, k):
        return w_copy(wot, w_group[o], 64, 8 + 3 * o + k - 1, (z_peer, y_peer)[o](k))

    def w_core():
        return w_copy(wot, core * 512, 512, 14, cpeer)

    w_all = [(o, k) for o in range(2) for k in (1, 2, 3)]

    def w_event0():
        for o in range(2):
            w_pair(o).wait_recv()
        for o, k in w_all:
            w_small(o, k).start()

    def w_event1():
        for o, k in w_all:
            w_small(o, k).wait_recv()
        for o, k in w_all:
            w_big(o, k).start()

    def w_event2():
        for o, k in w_all:
            w_big(o, k).wait_recv()
        w_core().start()

    for c in range(CHUNKS):
        tok_copy(c).start()
        if c == 0:
            w_pair(0).start()
            w_pair(1).start()

    def kv_copy(l, c, src_slot, dst_slot, send, recv, stage, target):
        return pltpu.make_async_remote_copy(
            src_ref=kv.at[l, src_slot, c], dst_ref=kv.at[l, dst_slot, c],
            send_sem=send.at[l, stage, c], recv_sem=recv.at[l, stage, c],
            device_id={"seq": target, "head": head}, device_id_type=mesh_id)

    def z_copy(l, c, i):
        return kv_copy(l, c, 4 * i, 4 * i + 4, zs, zr, i, nxt)

    def x_copy(l, c, i):
        return kv_copy(l, c, 4 * i + 4 * xlo, 4 * i + 2, xs, xr, i, xpeer)

    def o_copy(l, c, i):
        return kv_copy(l, c, 4 * i + 4 * core, 4 * i + 1 + 2 * core, os_, or_, i, cpeer)

    def c_copy(l, c, i):
        return kv_copy(l, c, 4 * i + 2, 4 * i + 3 - 2 * core, cs, cr, i, cpeer)

    def event0(l, c):
        z_copy(l, c, 0).start()

        @pl.when(xlo == 0)
        def _():
            x_copy(l, c, 0).start()

        @pl.when(core == 0)
        def _():
            o_copy(l, c, 0).start()

    def event1(l, c):
        z_copy(l, c, 0).wait_recv()
        z_copy(l, c, 1).start()

        @pl.when(xlo == 1)
        def _():
            x_copy(l, c, 0).start()

        @pl.when(xlo == 0)
        def _():
            x_copy(l, c, 1).start()

        @pl.when(core == 1)
        def _():
            o_copy(l, c, 0).start()

        @pl.when(core == 0)
        def _():
            o_copy(l, c, 1).start()

    def event2(l, c):
        x_copy(l, c, 0).wait_recv()
        c_copy(l, c, 0).start()

    def event3(l, c):
        z_copy(l, c, 1).wait_recv()

        @pl.when(xlo == 1)
        def _():
            x_copy(l, c, 1).start()

        @pl.when(core == 1)
        def _():
            o_copy(l, c, 1).start()

    def event4(l, c):
        x_copy(l, c, 1).wait_recv()
        c_copy(l, c, 1).start()

    cb, sb = cos_tab[pl.ds(seq, 1), :], sin_tab[pl.ds(seq, 1), :]
    ci, si = cos_tab[64:80, :], sin_tab[64:80, :]
    run_cos, run_sin = cb * ci - sb * si, sb * ci + cb * si
    cj, sj = cos_tab[80:112, :], sin_tab[80:112, :]
    sign = jnp.where(lax.broadcasted_iota(jnp.int32, (32, HEAD_SIZE), 1) < 64, -1.0, 1.0)
    for i in range(16):
        a, b = run_cos[i : i + 1, :], run_sin[i : i + 1, :]
        cos_ref[i * 32 : (i + 1) * 32, :] = a * cj - b * sj
        sin_ref[i * 32 : (i + 1) * 32, :] = (b * cj + a * sj) * sign

    own_count = counts[seq]
    lanes = lax.broadcasted_iota(jnp.int32, (16, ROWS), 1)
    sub = lax.broadcasted_iota(jnp.int32, (16, ROWS), 0)
    for d in range(SLOTS):
        n_valid = counts[lax.rem(seq + blocks - d, blocks)]
        vm[d] = jnp.where((lanes < n_valid) & (sub == 0), 1.0, 0.0).astype(jnp.bfloat16)
    far_count = counts[lax.rem(seq + blocks - 8, blocks)]

    def rope(val, cos, sin):
        return val * cos + pltpu.roll(val, 64, 1) * sin

    def project(l, c):
        rows = rc_rows(c)
        x0 = xb[0, rows, :].astype(jnp.float32)
        x1 = xb[1, rows, :].astype(jnp.float32)
        total = jnp.sum(x0 * x0, axis=1, keepdims=True) + jnp.sum(x1 * x1, axis=1, keepdims=True)
        factor = lax.rsqrt(total / MODEL_WIDTH + NORM_EPSILON)
        nb[:, 0:HALF] = (x0 * factor * gain[pl.ds(l, 1), 0:HALF]).astype(jnp.bfloat16)
        nb[:, HALF:] = (x1 * factor * gain[pl.ds(l, 1), HALF:]).astype(jnp.bfloat16)
        cos = cos_ref[rows, :]
        sin = sin_ref[rows, :]
        kvp = jnp.dot(nb[...], wkvb[l], preferred_element_type=jnp.float32)
        valid = lax.broadcasted_iota(jnp.int32, (CHUNK, HEAD_SIZE), 0) + c * CHUNK < own_count
        for g in range(2):
            key = rope(kvp[:, g * 128 : (g + 1) * 128], cos, sin).astype(jnp.bfloat16)
            if c > 0:
                first = kv[l, 0, 0, g * 128 : g * 128 + 1, :]
                key = jnp.where(valid, key.astype(jnp.float32), first.astype(jnp.float32)).astype(jnp.bfloat16)
            kv[l, 0, c, g * 128 : (g + 1) * 128, :] = key
            val = jnp.where(valid, kvp[:, 256 + g * 128 : 256 + (g + 1) * 128], 0.0)
            kv[l, 0, c, 256 + g * 128 : 256 + (g + 1) * 128, :] = val.T.astype(jnp.bfloat16)
        event0(l, c)
        for half in range(2):
            qp = jnp.dot(nb[...], wqb[l, :, half * 512 : (half + 1) * 512], preferred_element_type=jnp.float32)
            for h in range(4):
                rot = rope(qp[:, h * 128 : (h + 1) * 128], cos, sin) * QUERY_SCALE
                qs[half * 4 + c, h * 128 : (h + 1) * 128, :] = rot.astype(jnp.bfloat16)

    def keys_of(l, slot, g, lo, hi):
        return jnp.concatenate([kv[l, slot, c, g * 128 : (g + 1) * 128, :] for c in range(lo, hi)], axis=0)

    def values_of(l, slot, g, lo, hi):
        vt = jnp.concatenate([kv[l, slot, c, 256 + g * 128 : 256 + (g + 1) * 128, :] for c in range(lo, hi)], axis=1)
        return jnp.concatenate([vt, vm[slot, :, lo * 128 : hi * 128]], axis=0)

    def scores(l, slot, g, c, lo, hi):
        return lax.dot_general(keys_of(l, slot, g, lo, hi), qs[g * 4 + c], NT, preferred_element_type=jnp.float32)

    def sweep(l, tiles, mask=None, first=False):
        nxt_s = scores(l, *tiles[0])
        late = None

        def finish(slot, g, c, lo, hi, n, fade):
            u = g * 4 + c
            part = jnp.dot(values_of(l, slot, g, lo, hi), pbuf[n, 0 : (hi - lo) * 128, :], preferred_element_type=jnp.float32)
            acc[u] = part if fade is None else acc[u] * fade + part

        for n, tile in enumerate(tiles):
            slot, g, c, lo, hi = tile
            u = g * 4 + c
            s = nxt_s
            if n + 1 < len(tiles):
                nxt_s = scores(l, *tiles[n + 1])
            if late is not None:
                finish(*late)
            if mask is not None:
                key_at = lax.broadcasted_iota(jnp.int32, s.shape, 0) + lo * 128
                row_at = (lax.broadcasted_iota(jnp.int32, s.shape, 1) & 127) + c * CHUNK
                s = jnp.where(mask(key_at, row_at), s, LOW)
            m_new = jnp.max(s, axis=0, keepdims=True)
            fade = None
            if not first:
                m_old = m_ref[u]
                m_new = jnp.maximum(m_old, m_new)
                fade = jnp.exp2(m_old - m_new)
            pbuf[n % 2, 0 : (hi - lo) * 128, :] = jnp.exp2(s - m_new).astype(jnp.bfloat16)
            m_ref[u] = m_new
            late = (*tile, n % 2, fade)
        finish(*late)

    every = [(g, c) for g in range(2) for c in range(CHUNKS)]
    lane_slot = 3 - 2 * core
    cross_slot = 1 + 2 * core

    def attention(l):
        sweep(l, [(0, g, c, 0, c + 1) for g, c in every], lambda key_at, row_at: key_at <= row_at, True)

        @pl.when(l == 1)
        def _():
            event1(1, 2)
            event3(1, 1)

        event1(l, 3)

        def early(n, carry):
            @pl.when(n == 0)
            def _():
                event2(l, 0)
                event2(l, 1)
                event4(l, 0)
                event3(l, 2)

            @pl.when(n == 1)
            def _():
                event2(l, 2)
                event4(l, 1)
                event3(l, 3)
                for c in range(CHUNKS):
                    o_copy(l, c, 0).wait_recv()

            slot = jnp.where(n == 0, 4, lane_slot)

            @pl.when(seq >= slot)
            def _():
                sweep(l, [(slot, g, c, 0, 4) for g, c in every])

            return carry

        lax.fori_loop(0, 2, early, 0)
        event2(l, 3)
        event4(l, 2)

        @pl.when(seq >= 8)
        def _():
            sweep(l, [(8, g, c, c, 4) for g, c in every], lambda key_at, row_at: (key_at > row_at) & (key_at < far_count))

        event4(l, 3)
        for c in range(CHUNKS):
            c_copy(l, c, 0).wait_recv()
            o_copy(l, c, 1).wait_recv()
            c_copy(l, c, 1).wait_recv()

    def middle(l, c):
        @pl.when(seq >= 8)
        def _():
            sweep(l, [(slot, g, c, 0, 4) for slot in (cross_slot, 2, 5, 6, 7) for g in range(2)])

        @pl.when(seq < 8)
        def _():
            def one(n, carry):
                slot = jnp.where(n == 0, cross_slot, jnp.where(n == 1, 2, n + 3))

                @pl.when(seq >= slot)
                def _():
                    sweep(l, [(slot, g, c, 0, 4) for g in range(2)])

                return carry

            lax.fori_loop(0, 5, one, 0)

    def attended(c):
        for g in range(2):
            u = g * 4 + c
            norm = acc[u, 0:128, :] / acc[u, 128:129, :]
            for h in range(4):
                ab[c, :, (g * 4 + h) * 128 : (g * 4 + h + 1) * 128] = norm[:, h * 128 : (h + 1) * 128].T.astype(jnp.bfloat16)

    def full_copy(c):
        return pltpu.make_async_remote_copy(
            src_ref=ab.at[c], dst_ref=pr.at[c], send_sem=ps.at[0, c], recv_sem=pr_sem.at[0, c],
            device_id={"seq": seq, "head": pair}, device_id_type=mesh_id)

    def half_copy(c):
        return pltpu.make_async_remote_copy(
            src_ref=pb1.at[c], dst_ref=pr1.at[c], send_sem=ps.at[1, c], recv_sem=pr_sem.at[1, c],
            device_id={"seq": seq, "head": pair}, device_id_type=mesh_id)

    def early_events(l, c):
        @pl.when(l == 0)
        def _():
            if c >= 1:
                event1(0, c - 1)
            if c >= 2:
                event3(0, c - 2)
            if c == 1:
                w_event0()

        @pl.when(l == 1)
        def _():
            if c == 2:
                event1(1, 0)
            if c == 3:
                event1(1, 1)
                event3(1, 0)

    other_cols = pl.ds(pl.multiple_of(pair * HALF, HALF), HALF)
    own_cols = pl.ds(pl.multiple_of(head * HALF, HALF), HALF)

    def dots(l, c, cols):
        return jnp.dot(ab[c], wob[l, :, cols], preferred_element_type=jnp.float32).astype(jnp.bfloat16)

    def layer(l, carry):
        for c in range(CHUNKS):
            rows = rc_rows(c)

            @pl.when(l == 0)
            def _():
                if c == 0:
                    for load in loads[0:4]:
                        load.wait()
                tok_copy(c).wait_recv()

            @pl.when(l == 1)
            def _():
                if c == 0:
                    for load in loads[5:8]:
                        load.wait()
                    w_core().wait_recv()
                full_copy(c).wait_recv()
                for half in range(2):
                    cols = slice(half * HALF, (half + 1) * HALF)
                    arrived = jnp.dot(pr[c], wot[:, cols], preferred_element_type=jnp.float32).astype(jnp.bfloat16)
                    summed = pb[c, :, cols].astype(jnp.float32) + arrived.astype(jnp.float32)
                    xb[half, rows, :] = (xb[half, rows, :].astype(jnp.float32) + summed).astype(jnp.bfloat16)

            project(l, c)
            early_events(l, c)
        attention(l)

        @pl.when(l == 0)
        def _():
            w_event1()
            loads[4].wait()

        @pl.when(l == 1)
        def _():
            loads[8].wait()

        def chunk(c, carry):
            rows = pl.ds(pl.multiple_of(c * CHUNK, CHUNK), CHUNK)
            middle(l, c)

            @pl.when(l == 1)
            def _():
                full_copy(c).wait_send()

            attended(c)

            @pl.when(l == 0)
            def _():
                full_copy(c).start()
                for half in range(2):
                    pb[c, :, half * HALF : (half + 1) * HALF] = dots(0, c, pl.ds(half * HALF, HALF))

                @pl.when(c == 2)
                def _():
                    w_event2()

            @pl.when(l == 1)
            def _():
                pb1[c] = dots(1, c, other_cols)
                half_copy(c).start()
                out_ref[rows, :] = dots(1, c, own_cols)

            return carry

        return lax.fori_loop(0, CHUNKS, chunk, carry)

    lax.fori_loop(0, LAYER_COUNT, layer, 0)
    for c in range(CHUNKS):
        rows = rc_rows(c)
        half_copy(c).wait_recv()
        summed = out_ref[rows, :].astype(jnp.float32) + pr1[c].astype(jnp.float32)
        out_ref[rows, :] = (xb[head, rows, :].astype(jnp.float32) + summed).astype(jnp.bfloat16)

    w_pair(0).wait_send()
    w_pair(1).wait_send()
    w_core().wait_send()
    for o, k in w_all:
        w_small(o, k).wait_send()
        w_big(o, k).wait_send()
    for c in range(CHUNKS):
        tok_copy(c).wait_send()
        half_copy(c).wait_send()
        for l in range(LAYER_COUNT):
            for i in range(2):
                z_copy(l, c, i).wait_send()
                x_copy(l, c, i).wait_send()
                o_copy(l, c, i).wait_send()
                c_copy(l, c, i).wait_send()


def per_device(tokens, norm_gain, w_query, key_projection_weight, value_projection_weight, w_out, counts):
    blocks = lax.axis_size("seq")
    half_dim = HEAD_SIZE // 2
    inverse = ROPE_BASE ** (-2.0 * np.arange(half_dim) / HEAD_SIZE)
    offsets = np.concatenate([np.arange(64) * ROWS, np.arange(16) * 32, np.arange(32)])
    angles = np.tile(offsets[:, None] * inverse[None, :], (1, 2))
    cos2 = jnp.asarray(np.cos(angles), jnp.float32)
    sin2 = jnp.asarray(np.sin(angles), jnp.float32)
    bf16, f32 = jnp.bfloat16, jnp.float32
    any_, vmem = pl.BlockSpec(memory_space=pl.ANY), pl.BlockSpec(memory_space=pltpu.VMEM)
    dma = pltpu.SemaphoreType.DMA
    return pl.pallas_call(
        functools.partial(mega, blocks),
        out_shape=jax.ShapeDtypeStruct((ROWS, HALF), bf16),
        in_specs=[any_, vmem, any_, any_, any_, any_, vmem, vmem, pl.BlockSpec(memory_space=pltpu.SMEM)],
        out_specs=vmem,
        scratch_shapes=[
            pltpu.VMEM((ROWS, HEAD_SIZE), f32),
            pltpu.VMEM((ROWS, HEAD_SIZE), f32),
            pltpu.VMEM((2, ROWS, HALF), bf16),
            pltpu.VMEM((2, MODEL_WIDTH, HALF), bf16),
            pltpu.VMEM((2, MODEL_WIDTH, 512), bf16),
            pltpu.VMEM((2, HALF, MODEL_WIDTH), bf16),
            pltpu.VMEM((CHUNK, MODEL_WIDTH), bf16),
            pltpu.VMEM((8, 512, 128), bf16),
            pltpu.VMEM((2, SLOTS, CHUNKS, 512, 128), bf16),
            pltpu.VMEM((SLOTS, 16, ROWS), bf16),
            pltpu.VMEM((8, 1, 512), f32),
            pltpu.VMEM((8, 144, 512), f32),
            pltpu.VMEM((2, ROWS, 512), bf16),
            pltpu.VMEM((CHUNKS, CHUNK, HALF), bf16),
            pltpu.VMEM((CHUNKS, CHUNK, MODEL_WIDTH), bf16),
            pltpu.VMEM((CHUNKS, CHUNK, HALF), bf16),
            pltpu.VMEM((CHUNKS, CHUNK, HALF), bf16),
            pltpu.VMEM((CHUNKS, CHUNK, HALF), bf16),
            pltpu.VMEM((HALF, MODEL_WIDTH), bf16),
            dma((9,)), dma((4,)), dma((4,)),
            dma((2, 2, 4)), dma((2, 2, 4)), dma((2, 2, 4)), dma((2, 2, 4)),
            dma((2, 2, 4)), dma((2, 2, 4)), dma((2, 2, 4)), dma((2, 2, 4)),
            dma((2, 4)), dma((2, 4)), dma((15,)), dma((15,)),
        ],
        compiler_params=pltpu.CompilerParams(
            collective_id=0, has_side_effects=True, vmem_limit_bytes=63 * 2**20
        ),
    )(tokens, norm_gain, w_query, key_projection_weight, value_projection_weight, w_out, cos2, sin2, counts)


def solution(mesh):
    return jax.shard_map(
        per_device,
        mesh=mesh,
        in_specs=(
            P("seq", "head"),
            P(),
            P(None, None, "head"),
            P(None, None, "head"),
            P(None, None, "head"),
            P(None, "head", None),
            P(),
        ),
        out_specs=P("seq", "head"),
        check_vma=False,
    )
```
